32 devices in a mesh: dp: 4 (over y, core), seq: 8 (over z, x).
Axes of the slice: x: 2, y: 2, z: 4, core: 2. Of those that a mesh axis runs over, the one named last changes fastest.
Arguments:
- head_inputs: bfloat16 [4, 3072, 1024], P('dp', 'seq'), may hold values from -6 to 6
- gate_inputs: bfloat16 [4, 3072, 1024], P('dp', 'seq'), may hold values from -6 to 6
- state_proj: bfloat16 [4, 3072, 256], P('dp', 'seq'), may hold values from -2 to 2
- time_steps: float32 [4, 3072, 16], P('dp', 'seq'), may hold values from -4.7 to 4.7
- token_ids: int32 [4, 3072], P('dp', 'seq'), may hold values from 0 to 50279, as said below
- token_counts: int32 [4], replicated, may hold values from 1536 to 3072
- teacher_out: bfloat16 [4, 3072, 1024], P('dp', 'seq'), may hold values from -6 to 6
- out_weight: float32 [1024, 1024], P(('dp', 'seq')), may hold values from -0.1875 to 0.1875
- decay_log: float32 [16], replicated, may hold values from -6.5 to 1
- step_bias: float32 [16], replicated, may hold values from -5 to -3
- skip_gain: float32 [16], replicated, may hold values from 0.5 to 1.5
- norm_gain: float32 [1024], replicated, may hold values from 0.5 to 1.5
Outputs:
- losses: float32 [2], replicated
- new_weight: float32 [1024, 1024], P(('dp', 'seq'))
- new_decay: float32 [16], replicated
- new_bias: float32 [16], replicated
- new_skip: float32 [16], replicated
- new_gain: float32 [1024], replicated
The draws below stay inside these ranges and needn't reach their ends.
Inputs may be any that keep to these rules, and one draw needn't show every extreme that they name: `token_ids`: in each sequence exactly one position, never the first, holds id 0.
All inputs are finite; a program needn't handle non-finite values.
Results may differ from the reference program's by a relative error of at most 0.0003.
Values may be sent and summed in bfloat16 or wider, within the bound.
No kernel may reach another device: no remote copies, remote signals or barrier semaphores. Data moves between devices by JAX's collectives and lax.ppermute only.
A program may use at most 192 MiB of HBM per device.

```python
import jax
import jax.numpy as jnp
from jax import lax

D = 1024
N = 128
VOCAB = 50280
H = 16
STEPS = 2
TOK_DEV = 384
SEQS = 4
LENGTH = 3072
DI = 1024
N_SEQ = 8


def draw_time_steps(key, part):
    noise_key, shift_key = jax.random.split(key)
    blocks = LENGTH // TOK_DEV
    offset = jax.random.uniform(shift_key, (SEQS, blocks, 1, H), jnp.float32, -0.7, 0.7)
    jitter = jnp.clip(jax.random.normal(noise_key, (SEQS, blocks, TOK_DEV, H), jnp.float32), -4.0, 4.0)
    return (jitter + offset).reshape(SEQS, LENGTH, H)


def draw_decay_log(key, part):
    pick_key, strong_key, weak_key = jax.random.split(key, 3)
    strong = jax.random.randint(pick_key, (H,), 0, 2) > 0
    slow_rate = jax.random.uniform(strong_key, (H,), jnp.float32, -6.5, -5.5)
    quick_rate = jax.random.uniform(weak_key, (H,), jnp.float32, 0.0, 1.0)
    return jnp.where(strong, slow_rate, quick_rate)


def draw_token_ids(key, part):
    token_key, reset_key = jax.random.split(key)
    token_draw = jax.random.randint(token_key, (SEQS, LENGTH), 1, VOCAB)
    reset_at = jax.random.randint(reset_key, (SEQS, 1), 1, LENGTH)
    return jnp.where(jnp.arange(LENGTH)[None, :] == reset_at, 0, token_draw).astype(jnp.int32)


def plant(drawn, stream_key, low, largest):
    place = [jax.random.randint(jax.random.fold_in(stream_key, axis), (), 0, length) for axis, length in enumerate(drawn.shape)]
    main_axis = drawn.shape.index(max(drawn.shape))
    beside = place[:main_axis] + [(place[main_axis] + 1) % drawn.shape[main_axis]] + place[main_axis + 1:]
    return drawn.at[tuple(place)].set(low).at[tuple(beside)].set(largest)


def spiked(result, own_key, source, target, parts, factor):
    owner, partner = [(jnp.arange(result.shape[axis_at]) // (result.shape[axis_at] // parts)).reshape([-1 if axis == axis_at else 1 for axis in range(result.ndim)]) for axis_at in (source, target)]
    chosen = jax.random.permutation(own_key, parts)[partner]
    strong = (owner == chosen) | (owner == (partner + parts // 2) % parts)
    return jnp.where(strong, factor * result, result)


def steps_of(own_key, dims, cuts, least, high):
    factor_of, own = 1.0, jax.random.fold_in(own_key, 6)
    for axis_at, blocks in cuts:
        steps = jnp.exp(jax.random.uniform(jax.random.fold_in(own, axis_at), (blocks,), jnp.float32, least / len(cuts), high / len(cuts)))
        factor_of = factor_of * jnp.repeat(steps, dims[axis_at] // blocks).reshape([-1 if axis == axis_at else 1 for axis in range(len(dims))])
    return factor_of


def scatter_about(stream_key, shape, scale, reach, cuts=(), kind=jnp.bfloat16):
    result = jax.random.normal(stream_key, shape, jnp.float32) * scale
    if len(cuts) > 0:
        result = steps_of(stream_key, shape, cuts, -0.22, 0.18) * result
    return jnp.clip(result, min=-reach, max=reach).astype(kind)


def gaussian_with(key, dims, scale, bound, cuts, heavy, dtype=jnp.bfloat16):
    entries = scale * jax.random.normal(key, dims, jnp.float32)
    if cuts:
        entries = entries * steps_of(key, dims, cuts, -0.22, 0.18)
    return jnp.clip(spiked(entries, jax.random.fold_in(key, 3), *heavy), -bound, bound).astype(dtype)


def setup_inputs(seed: int = 0) -> dict:
    arg_keys = jax.random.split(jax.random.key(seed), 13)
    return {
        "head_inputs": scatter_about(arg_keys[0], (SEQS, LENGTH, DI), 1.0, 6.0, ((0, 4), (1, 8))),
        "gate_inputs": gaussian_with(arg_keys[1], (SEQS, LENGTH, DI), 1.0, 6.0, ((0, 4), (1, 8)), (1, 2, 8, 2.0)),
        "state_proj": scatter_about(arg_keys[2], (SEQS, LENGTH, 2 * N), 0.3, 2.0, ((0, 4), (1, 8))),
        "time_steps": draw_time_steps(jax.random.fold_in(arg_keys[12], 71), 0),
        "token_ids": draw_token_ids(jax.random.fold_in(arg_keys[12], 71), 0),
        "token_counts": plant(jax.random.randint(arg_keys[5], (SEQS,), LENGTH // 2, LENGTH + 1), jax.random.fold_in(arg_keys[5], 1), LENGTH // 2, LENGTH).astype(jnp.int32),
        "teacher_out": scatter_about(arg_keys[6], (SEQS, LENGTH, D), 1.0, 6.0, ((0, 4), (1, 8))),
        "out_weight": scatter_about(arg_keys[7], (DI, D), DI ** -0.5, 0.1875, ((0, 32),), jnp.float32),
        "decay_log": draw_decay_log(jax.random.fold_in(arg_keys[12], 71), 0),
        "step_bias": jnp.clip(jax.random.uniform(arg_keys[9], (H,), jnp.float32, -5.0, -3.0), -5.0, -3.0),
        "skip_gain": jnp.clip(jax.random.uniform(arg_keys[10], (H,), jnp.float32, 0.5, 1.5), 0.5, 1.5),
        "norm_gain": jnp.clip(1.0 + 0.1 * jax.random.normal(arg_keys[11], (DI,), jnp.float32), 0.5, 1.5),
    }


norm_floor = 1.0
clip_limit = 1.0
learn_rate = 8.0
highest = lax.Precision.HIGHEST
masked_low = -10000.0

def step_sizes(decay_log, step_bias, step_raw):
    step_width = jax.nn.softplus(step_raw + step_bias[None, :])
    decay_sum = jnp.cumsum(step_width * (-jnp.exp(decay_log))[None, :], axis=0)
    return (step_width, decay_sum)

def mix_block(decay_log, step_bias, skip_gain, norm_gain, state_in, head_inputs, gate_inputs, b_proj, c_proj, step_raw, segment):
    positions = head_inputs.shape[0]
    head_count = decay_log.shape[0]
    step_width, decay_sum = step_sizes(decay_log, step_bias, step_raw)
    inputs_f = head_inputs.astype(jnp.float32).reshape(positions, head_count, -1)
    scaled = inputs_f * step_width[:, :, None]
    scores = jnp.dot(c_proj, b_proj.T, preferred_element_type=jnp.float32)
    position = jnp.arange(positions)
    allowed = (segment[:, None] == segment[None, :]) & (position[:, None] >= position[None, :])

    def one_head(head_data):
        head_sum, head_scaled = head_data
        spread = head_sum[:, None] - head_sum[None, :]
        decay_grid = jnp.exp(jnp.where(allowed, spread, masked_low))
        return jnp.dot(decay_grid * scores, head_scaled, precision=highest)
    intra_sum = jnp.transpose(lax.map(one_head, (decay_sum.T, jnp.transpose(scaled, (1, 0, 2)))), (1, 0, 2))
    entry_decay = jnp.exp(decay_sum) * (segment == 0)[:, None]
    carried = jnp.einsum('in,hpn->ihp', c_proj.astype(jnp.float32), state_in, precision=highest) * entry_decay[:, :, None]
    mixed_out = intra_sum + carried + skip_gain[None, :, None] * inputs_f
    gated = mixed_out.reshape(positions, -1) * jax.nn.silu(gate_inputs.astype(jnp.float32))
    mean_square = lax.optimization_barrier(jnp.mean(gated * gated, axis=1, keepdims=True))
    return gated * norm_gain[None, :] * lax.rsqrt(mean_square + norm_floor)

def state_block(decay_log, step_bias, head_inputs, b_proj, step_raw, segment):
    positions = head_inputs.shape[0]
    head_count = decay_log.shape[0]
    step_width, decay_sum = step_sizes(decay_log, step_bias, step_raw)
    final_sum = decay_sum[-1]
    same_doc = (segment == segment[-1])[:, None]
    tail_decay = jnp.exp(jnp.where(same_doc, final_sum[None, :] - decay_sum, masked_low))
    inputs_f = head_inputs.astype(jnp.float32).reshape(positions, head_count, -1)
    weighted = inputs_f * (step_width * tail_decay)[:, :, None]
    state_out = jnp.einsum('jhp,jn->hpn', weighted, b_proj.astype(jnp.float32), precision=highest)
    carry_out = jnp.exp(final_sum) * (segment[-1] == 0)
    return (carry_out, state_out)

def kahan_total(partials):

    def add_one(running, element):
        summed_up, correction = running
        adjusted = element - correction
        new_total = summed_up + adjusted
        correction = new_total - summed_up - adjusted
        return ((new_total, correction), None)
    (summed_up, correction), _ = lax.scan(add_one, (jnp.zeros((), jnp.float32), jnp.zeros((), jnp.float32)), partials)
    return summed_up

def reference(head_inputs, gate_inputs, state_proj, time_steps, token_ids, token_counts, teacher_out, out_weight, decay_log, step_bias, skip_gain, norm_gain):
    seq_count, length, inner_width = head_inputs.shape
    state_size = state_proj.shape[2] // 2
    model_width = teacher_out.shape[2]
    blocks = N_SEQ
    block_len = length // blocks
    head_count = decay_log.shape[0]
    head_size = inner_width // head_count

    def split_blocks(array):
        return array.reshape((seq_count, blocks, block_len) + array.shape[2:])
    starts = (token_ids == 0).astype(jnp.int32)
    segments = jnp.cumsum(split_blocks(starts), axis=2).astype(jnp.int32)
    position = jnp.arange(length).astype(jnp.int32)
    scored_all = (position[None, :] < token_counts[:, None]).astype(jnp.float32)
    total_count = jnp.sum(token_counts).astype(jnp.float32)
    pieces = (split_blocks(head_inputs), split_blocks(gate_inputs), split_blocks(state_proj), split_blocks(time_steps), segments)
    losses = []
    for step_index in range(STEPS):
        weight_b = out_weight.astype(jnp.bfloat16)
        params = (decay_log, step_bias, skip_gain, norm_gain)

        def one_sequence(running, seq_data):
            sequence, target_s, scored_s = seq_data

            def forward(params_in):

                def per_block(state_in, block_data):
                    inputs_b, gates_b, proj_b, raw_b, seg_b = block_data
                    normed_blk = mix_block(params_in[0], params_in[1], params_in[2], params_in[3], state_in, inputs_b, gates_b, proj_b[:, :state_size], proj_b[:, state_size:], raw_b, seg_b)
                    carry_out, state_out = state_block(params_in[0], params_in[1], inputs_b, proj_b[:, :state_size], raw_b, seg_b)
                    return (carry_out[:, None, None] * state_in + state_out, normed_blk)
                start_state = jnp.zeros((head_count, head_size, state_size), jnp.float32)
                _, normed_seq = lax.scan(jax.checkpoint(per_block), start_state, sequence)
                return normed_seq
            normed, pull_back = jax.vjp(forward, params)
            normed_b = normed.astype(jnp.bfloat16).reshape(-1, inner_width)
            output = jnp.dot(normed_b, weight_b, preferred_element_type=jnp.float32)
            residual = output - target_s.astype(jnp.float32)
            token_loss = lax.optimization_barrier(jnp.sum(residual * residual, axis=1)) * scored_s / model_width
            block_sums = lax.optimization_barrier(jnp.sum(token_loss.reshape(blocks, block_len), axis=1))
            out_grad = (residual * (2.0 / (model_width * total_count)) * scored_s[:, None]).astype(jnp.bfloat16)
            weight_part = jnp.dot(normed_b.T, out_grad, preferred_element_type=jnp.float32)
            normed_grad = jnp.dot(out_grad, weight_b.T, preferred_element_type=jnp.float32).reshape(normed.shape)
            small_part, = pull_back(normed_grad)
            new_running = (running[0] + weight_part, tuple((left + right for left, right in zip(running[1], small_part))))
            return (new_running, block_sums)
        start_running = (jnp.zeros(out_weight.shape, jnp.float32), tuple((jnp.zeros(member.shape, jnp.float32) for member in params)))
        (weight_grad, small_grads), partial_sums = lax.scan(one_sequence, start_running, (pieces, teacher_out, scored_all))
        losses.append(kahan_total(partial_sums.reshape(-1)) / total_count)
        norm_square = jnp.sum(weight_grad * weight_grad) + sum((jnp.sum(member * member) for member in small_grads))
        factor = clip_limit / jnp.maximum(jnp.sqrt(norm_square), clip_limit)
        out_weight = out_weight - learn_rate * factor * weight_grad
        decay_log = decay_log - learn_rate * factor * small_grads[0]
        step_bias = step_bias - learn_rate * factor * small_grads[1]
        skip_gain = skip_gain - learn_rate * factor * small_grads[2]
        norm_gain = norm_gain - learn_rate * factor * small_grads[3]
    return (jnp.stack(losses), out_weight, decay_log, step_bias, skip_gain, norm_gain)
```

```python
import jax
import jax.numpy as jnp
from jax import lax
from jax.experimental import pallas as pl
from jax.experimental.pallas import tpu as pltpu
from jax.sharding import PartitionSpec as P

STEPS = 2


norm_floor = 1.0
clip_limit = 1.0
learn_rate = 8.0
highest = lax.Precision.HIGHEST
masked_low = -10000.0
bf16 = jnp.bfloat16
f32 = jnp.float32


def decay_matmul(left, right, sum_cols, sum_rows, seg_col, seg_row, values, reverse):
    tokens, width = values.shape
    heads = sum_cols.shape[1]
    head_size = width // heads
    group = max(1, 128 // head_size)
    lanes = group * head_size

    def kernel(left_ref, right_ref, cols_ref, rows_ref, sc_ref, sr_ref, val_ref, out_ref):
        scores = lax.dot_general(
            left_ref[...], right_ref[...], (((1,), (1,)), ((), ())), preferred_element_type=f32
        )
        row = lax.broadcasted_iota(jnp.int32, (tokens, tokens), 0)
        col = lax.broadcasted_iota(jnp.int32, (tokens, tokens), 1)
        order = (col >= row) if reverse else (row >= col)
        allowed = order & (sc_ref[...] == sr_ref[...])
        scores = jnp.where(allowed, scores, 0.0)
        lane = lax.broadcasted_iota(jnp.int32, (tokens, lanes), 1)
        for base in range(0, heads, group):
            piece = val_ref[:, base * head_size : base * head_size + lanes]
            result = None
            for inner in range(group):
                head = base + inner
                spread = cols_ref[:, head : head + 1] - rows_ref[head : head + 1, :]
                if reverse:
                    spread = -spread
                grid = (jnp.exp(jnp.minimum(spread, 0.0)) * scores).astype(bf16)
                part = jnp.dot(grid, piece, preferred_element_type=f32)
                result = part if result is None else jnp.where(lane >= inner * head_size, part, result)
            out_ref[:, base * head_size : base * head_size + lanes] = result

    return pl.pallas_call(
        kernel,
        out_shape=jax.ShapeDtypeStruct((tokens, width), f32),
        name="decay_back" if reverse else "decay_ahead",
    )(left, right, sum_cols, sum_rows, seg_col, seg_row, values)


def per_device(
    head_inputs,
    gate_inputs,
    state_proj,
    time_steps,
    token_ids,
    token_counts,
    teacher_out,
    out_weight,
    decay_log,
    step_bias,
    skip_gain,
    norm_gain,
):
    tok_rows = head_inputs.shape[1]
    inner_width = head_inputs.shape[2]
    state_size = state_proj.shape[2] // 2
    model_width = teacher_out.shape[2]
    head_count = decay_log.shape[0]
    head_size = inner_width // head_count
    blocks = lax.axis_size("seq")
    place = lax.axis_index("seq")
    x_b = head_inputs[0]
    x_f = x_b.astype(f32)
    b_proj = state_proj[0, :, :state_size]
    c_proj = state_proj[0, :, state_size:]
    raw = time_steps[0]
    token = jnp.arange(tok_rows, dtype=jnp.int32)
    starts = (token_ids[0] == 0).astype(jnp.int32)
    later = token[:, None] >= token[None, :]
    seg_col = jnp.sum(jnp.where(later, starts[None, :], 0), axis=1)[:, None]
    seg_row = jnp.sum(jnp.where(later.T, starts[:, None], 0), axis=0)[None, :]
    resets = jnp.sum(starts)
    lower = later.astype(f32)
    before_reset = (seg_col == 0).astype(f32)
    last_doc = seg_col == resets
    position = place * tok_rows + token
    own_count = lax.dynamic_index_in_dim(token_counts, lax.axis_index("dp"), keepdims=False)
    scored = (position < own_count).astype(f32)
    total_count = jnp.sum(token_counts).astype(f32)
    target_f = teacher_out[0].astype(f32)
    gate_f = gate_inputs[0].astype(f32)
    silu_gate = gate_f * jax.nn.sigmoid(gate_f)
    spread_mat = (
        jnp.arange(inner_width)[None, :] // head_size == jnp.arange(head_count)[:, None]
    ).astype(f32)

    def widen(a):
        return jnp.dot(a, spread_mat, precision=highest)

    def by_head(a):
        return lax.dot_general(a, spread_mat, (((1,), (1,)), ((), ())), precision=highest)

    index = jnp.arange(blocks)
    ahead_mask = (index[None, :] > index[:, None]) & (index[None, :] < place)
    back_mask = (index[None, :] < index[:, None]) & (index[None, :] > place)

    def block_weights(mask, valid, sums, counts):
        log_w = jnp.sum(jnp.where(mask[:, :, None], sums[None], 0.0), axis=1)
        hits = jnp.sum(jnp.where(mask, counts[None, :], 0.0), axis=1)
        return jnp.exp(log_w) * (valid & (hits == 0.0))[:, None].astype(f32)

    losses = []
    for step_index in range(STEPS):
        weight_all = lax.all_gather(out_weight.astype(bf16), ("dp", "seq"), axis=0, tiled=True)
        shifted = raw + step_bias[None, :]
        width = jax.nn.softplus(shifted)
        rate = width * (-jnp.exp(decay_log))[None, :]
        decay_sum = jnp.dot(lower, rate, precision=highest)
        sum_rows = decay_sum.T
        final_sum = decay_sum[-1]
        tail = jnp.exp(jnp.where(last_doc, final_sum[None, :] - decay_sum, masked_low))
        entry = widen(jnp.exp(decay_sum) * before_reset)
        width_wide = widen(width)
        tail_wide = widen(tail)
        scaled_f = x_f * width_wide
        scaled = scaled_f.astype(bf16)
        weighted = (scaled_f * tail_wide).astype(bf16)
        state_out = lax.dot_general(
            weighted, b_proj, (((0,), (0,)), ((), ())), preferred_element_type=f32
        )
        high = final_sum.astype(bf16)
        rest = final_sum - high.astype(f32)
        mid = rest.astype(bf16)
        low = (rest - mid.astype(f32)).astype(bf16)
        count_b = jnp.full((head_count,), resets, f32).astype(bf16)
        meta = jnp.stack([high, mid, low, count_b], axis=1)
        meta = jnp.pad(meta, ((0, 0), (0, state_size - 4)))
        gathered = lax.all_gather(jnp.concatenate([state_out.astype(bf16), meta], axis=0), "seq")
        meta_all = gathered[:, inner_width:, :4].astype(f32)
        sums_all = meta_all[:, :, 0] + meta_all[:, :, 1] + meta_all[:, :, 2]
        counts_all = meta_all[:, 0, 3]
        intra = decay_matmul(
            c_proj, b_proj, decay_sum, sum_rows, seg_col, seg_row, scaled, False
        )
        ahead = block_weights(ahead_mask, index < place, sums_all, counts_all)
        states = gathered[:, :inner_width].reshape(blocks, head_count, head_size, state_size)
        state_in = jnp.sum(states.astype(f32) * ahead[:, :, None, None], axis=0)
        state_in_b = state_in.reshape(inner_width, state_size).astype(bf16)
        carried = entry * lax.dot_general(
            c_proj, state_in_b, (((1,), (1,)), ((), ())), preferred_element_type=f32
        )
        mixed = intra + carried
        gated = (mixed + widen(skip_gain[None, :]) * x_f) * silu_gate
        scale = lax.rsqrt(jnp.mean(gated * gated, axis=1, keepdims=True) + norm_floor)
        unit = gated * scale
        normed_b = (unit * norm_gain[None, :]).astype(bf16)
        output = jnp.dot(normed_b, weight_all, preferred_element_type=f32)
        residual = output - target_f
        loss_part = jnp.sum(jnp.sum(residual * residual, axis=1) * scored) / model_width
        out_grad = (residual * (2.0 / (model_width * total_count)) * scored[:, None]).astype(bf16)
        weight_grad = lax.dot_general(
            normed_b, out_grad, (((0,), (0,)), ((), ())), preferred_element_type=f32
        )
        grad_rows = lax.psum_scatter(weight_grad, ("dp", "seq"), scatter_dimension=0, tiled=True)
        normed_grad = lax.dot_general(
            out_grad, weight_all, (((1,), (1,)), ((), ())), preferred_element_type=f32
        )
        gain_grad = jnp.sum(normed_grad * unit, axis=0)
        unit_grad = normed_grad * norm_gain[None, :]
        gated_grad = scale * (
            unit_grad - unit * jnp.mean(unit_grad * unit, axis=1, keepdims=True)
        )
        mixed_grad_f = gated_grad * silu_gate
        mixed_grad = mixed_grad_f.astype(bf16)
        rounded = mixed_grad.astype(f32)
        state_grad = lax.dot_general(
            (mixed_grad_f * entry).astype(bf16),
            c_proj,
            (((0,), (0,)), ((), ())),
            preferred_element_type=f32,
        )
        grads_all = lax.all_gather(state_grad.astype(bf16), "seq")
        intra_back = decay_matmul(
            b_proj, c_proj, decay_sum, sum_rows, seg_col, seg_row, mixed_grad, True
        )
        skip_grad = jnp.sum(by_head(jnp.sum(mixed_grad_f * x_f, axis=0, keepdims=True)), axis=0)
        back = block_weights(back_mask, index > place, sums_all, counts_all)
        grads_all = grads_all.reshape(blocks, head_count, head_size, state_size)
        after = jnp.sum(grads_all.astype(f32) * back[:, :, None, None], axis=0)
        carry_out = jnp.exp(final_sum) * (resets == 0)
        carry_grad = jnp.sum(after * state_in, axis=(1, 2)) * carry_out
        from_after = tail_wide * lax.dot_general(
            b_proj,
            after.reshape(inner_width, state_size).astype(bf16),
            (((1,), (1,)), ((), ())),
            preferred_element_type=f32,
        )
        back_near = by_head(intra_back * scaled.astype(f32))
        back_far = by_head(from_after * scaled_f)
        width_grad = by_head((intra_back + from_after) * x_f)
        sum_grad = by_head(rounded * mixed) - back_near - back_far
        rate_grad = lax.dot_general(lower, sum_grad, (((0,), (0,)), ((), ())), precision=highest)
        rate_grad = rate_grad + (jnp.sum(back_far, axis=0) + carry_grad)[None, :]
        decay_grad = jnp.sum(rate_grad * rate, axis=0)
        width_grad = width_grad + rate_grad * (-jnp.exp(decay_log))[None, :]
        bias_grad = jnp.sum(width_grad * jax.nn.sigmoid(shifted), axis=0)
        packed = jnp.concatenate(
            [
                gain_grad,
                decay_grad,
                bias_grad,
                skip_grad,
                jnp.sum(grad_rows * grad_rows)[None],
                loss_part[None],
            ]
        )
        merged = lax.psum(packed, ("dp", "seq"))
        small = merged[: inner_width + 3 * head_count]
        norm_square = merged[inner_width + 3 * head_count] + jnp.sum(small * small)
        losses.append(merged[inner_width + 3 * head_count + 1] / total_count)
        factor = clip_limit / jnp.maximum(jnp.sqrt(norm_square), clip_limit)
        change = learn_rate * factor
        out_weight = out_weight - change * grad_rows
        small = change * small
        norm_gain = norm_gain - small[:inner_width]
        decay_log = decay_log - small[inner_width : inner_width + head_count]
        step_bias = step_bias - small[inner_width + head_count : inner_width + 2 * head_count]
        skip_gain = skip_gain - small[inner_width + 2 * head_count :]
    return (jnp.stack(losses), out_weight, decay_log, step_bias, skip_gain, norm_gain)

def solution(mesh):
    in_specs = (
        P("dp", "seq", None),
        P("dp", "seq", None),
        P("dp", "seq", None),
        P("dp", "seq", None),
        P("dp", "seq"),
        P(),
        P("dp", "seq", None),
        P(("dp", "seq"), None),
        P(),
        P(),
        P(),
        P(),
    )
    out_specs = (P(), P(("dp", "seq"), None), P(), P(), P(), P())
    return jax.shard_map(
        per_device, mesh=mesh, in_specs=in_specs, out_specs=out_specs, check_vma=False
    )
```
